32 devices in a mesh: gx: 4 (over x, core), gy: 4 (over z), gz: 2 (over y).
Axes of the slice: x: 2, y: 2, z: 4, core: 2. Of those that a mesh axis runs over, the one named last changes fastest.
Arguments:
- estimate: float32 [32, 64, 512], P('gz', 'gx', 'gy'), may hold values from 0.5 to 2
- measured: float32 [32, 64, 512], P('gz', 'gx', 'gy'), may hold values from 0.1 to 10
- point_spread: float32 [32, 1024], replicated, may hold values from 0.0005 to 4.01, as said below
Outputs:
- updated: float32 [32, 64, 512], P('gz', 'gx', 'gy')
- mip_x: float32 [32, 512], P('gz', 'gy')
- mip_y: float32 [32, 64], P('gz', 'gx')
- mip_z: float32 [64, 512], P('gx', ('gy', 'gz'))
The draws below stay inside these ranges and needn't reach their ends.
Inputs may be any that keep to these rules, and one draw needn't show every extreme that they name: `point_spread`: every entry is positive.
All inputs are finite; a program needn't handle non-finite values.
Results may differ from the reference program's by a relative error of at most 0.000076.
Values sent between devices are 32-bit elements; how exact they have to be, the bound alone decides.
No kernel may reach another device: no remote copies, remote signals or barrier semaphores. Data moves between devices by JAX's collectives and lax.ppermute only.
A program may use at most 64 MiB of HBM per device.

```python
import math
import jax
import jax.numpy as jnp

KERNEL = 32
HALF = 16
NZ = 32
NX = 64
NY = 512


def draw_point_spread(key, part):
    offsets = jnp.arange(KERNEL, dtype=jnp.float32) - KERNEL // 2
    along_z = offsets[:, None, None]
    along_x = offsets[None, :, None]
    along_y = offsets[None, None, :]
    core = jnp.exp(-(along_z * along_z / 8.0 + along_x * along_x / 2.0 + along_y * along_y / 2.0))
    factor = jnp.exp(jax.random.uniform(key, (KERNEL, KERNEL, KERNEL), jnp.float32, math.log(0.25), math.log(4.0)))
    return ((core + 0.002) * factor).reshape(KERNEL, KERNEL * KERNEL)


def block_scale(stream_key, extent, split, low, top_value):
    level, own = 1.0, jax.random.fold_in(stream_key, 6)
    for dim, parts in split:
        heights = jnp.exp(jax.random.uniform(jax.random.fold_in(own, dim), (parts,), jnp.float32, low / len(split), top_value / len(split)))
        level = level * jnp.repeat(heights, extent[dim] // parts).reshape([-1 if axis == dim else 1 for axis in range(len(extent))])
    return level


def setup_inputs(seed: int = 0) -> dict:
    key_list = jax.random.split(jax.random.key(seed), 4)
    estimate = jnp.clip(jnp.exp(math.log(2.0) - 1.3862944 * jax.random.uniform(key_list[0], (NZ, NX, NY), jnp.float32) ** block_scale(key_list[0], (NZ, NX, NY), ((0, 2), (1, 4), (2, 4)), -0.2, 0.2)), 0.5, 2.0)
    measured = jnp.clip(jnp.exp(math.log(10.0) - 4.6051702 * jax.random.uniform(key_list[1], (NZ, NX, NY), jnp.float32) ** block_scale(key_list[1], (NZ, NX, NY), ((0, 2), (1, 4), (2, 4)), -0.2, 0.2)), 0.1, 10.0)
    point_spread = draw_point_spread(jax.random.fold_in(key_list[3], 71), 0)
    return dict(estimate=estimate, measured=measured, point_spread=point_spread)


def reference(estimate, measured, point_spread):
    psf_cube = point_spread.reshape(KERNEL, KERNEL, KERNEL)
    psf_norm = psf_cube / jnp.sum(psf_cube)
    shape_all = (NZ + KERNEL, NX + KERNEL, NY + KERNEL)
    kernel_grid = jnp.pad(psf_norm, ((0, NZ), (0, NX), (0, NY)))
    kernel_grid = jnp.roll(kernel_grid, (-HALF, -HALF, -HALF), axis=(0, 1, 2))
    spectrum = jnp.fft.rfftn(kernel_grid)
    blurred = jnp.fft.irfftn(jnp.fft.rfftn(estimate, s=shape_all) * spectrum, s=shape_all)[:NZ, :NX, :NY]
    ratio = measured / blurred
    correction = jnp.fft.irfftn(jnp.fft.rfftn(ratio, s=shape_all) * jnp.conj(spectrum), s=shape_all)[:NZ, :NX, :NY]
    updated = estimate * correction
    return updated, jnp.max(updated, axis=1), jnp.max(updated, axis=2), jnp.max(updated, axis=0)
```

```python
import functools

import jax
import jax.numpy as jnp
import numpy as np
from jax import lax
from jax.experimental import pallas as pl
from jax.experimental.pallas import tpu as pltpu
from jax.sharding import PartitionSpec as P

F32 = jnp.float32
BF16 = jnp.bfloat16


def split(value):
    high = value.astype(BF16)
    return high, (value - high.astype(F32)).astype(BF16)


def constant(table):
    table = np.asarray(table, np.float32)
    high = table.astype(BF16)
    low = (table - high.astype(np.float32)).astype(BF16)
    return jnp.asarray(high), jnp.asarray(low)


def dot3(left, right):
    mul = functools.partial(jnp.dot, preferred_element_type=F32)
    return mul(left[0], right[0]) + (mul(left[0], right[1]) + mul(left[1], right[0]))


def angles(rows, cols, length):
    return np.mod(np.outer(rows, cols), length) * (2.0 * np.pi / length)


def forward_left(length, positions):
    theta = angles(np.arange(length), positions, length)
    c, s = np.cos(theta), np.sin(theta)
    return np.block([[c, s], [-s, c]])


def inverse_left(length, positions):
    theta = angles(positions, np.arange(length), length)
    c, s = np.cos(theta), np.sin(theta)
    return np.block([[c, -s], [s, c]])


def forward_right(length, positions, lanes):
    count = length // 2 + 1
    theta = angles(positions, np.arange(count), length)
    out = np.zeros((len(positions), 2 * lanes))
    out[:, :count] = np.cos(theta)
    out[:, lanes : lanes + count] = -np.sin(theta)
    return out


def inverse_right(length, positions, lanes):
    count = length // 2 + 1
    freq = np.arange(count)
    weight = np.where((freq == 0) | (2 * freq == length), 1.0, 2.0)[:, None]
    theta = angles(freq, positions, length)
    out = np.zeros((2 * lanes, len(positions)))
    out[:count] = weight * np.cos(theta)
    out[lanes : lanes + count] = -weight * np.sin(theta)
    return out


def pair_x(s1, row, rows, lanes):
    block = s1[pl.ds(row, rows), :]
    return jnp.concatenate([block[:, :lanes], block[:, lanes:]], axis=0)


def pair_strided(ref, start, gap, rows, stride):
    return jnp.concatenate(
        [ref[pl.ds(start, rows, stride=stride), :], ref[pl.ds(start + gap, rows, stride=stride), :]], axis=0
    )


def transform_x(s1, s2, table, count_z, count_x, length_x, lanes):
    def step(i, carry):
        z = i * 2
        data = jnp.concatenate(
            [pair_x(s1, (z + j) * count_x, count_x, lanes) for j in range(2)], axis=1
        )
        out = dot3(table, split(data))
        for j in range(2):
            s2[pl.ds((z + j) * 2 * length_x, 2 * length_x), :] = out[:, j * lanes : (j + 1) * lanes]
        return carry

    lax.fori_loop(0, count_z // 2, step, 0, unroll=4)


def spectrum_body(psf, ty_h, ty_l, fx_h, fx_l, fz_h, fz_l, spec, s1, s2, *, extent, dims, lanes):
    length_z, length_x, length_y = dims
    values = psf[...]
    scale = 1.0 / (jnp.sum(values) * float(length_z * length_x * length_y))
    s1[...] = dot3(split(values), (ty_h[...], ty_l[...])) * scale
    transform_x(s1, s2, (fx_h[...], fx_l[...]), extent, extent, length_x, lanes)
    table = (fz_h[...], fz_l[...])

    def step(i, carry):
        k = i * 2
        data = jnp.concatenate(
            [pair_strided(s2, k + j, length_x, extent, 2 * length_x) for j in range(2)], axis=1
        )
        out = dot3(table, split(data))
        for j in range(2):
            spec[pl.ds((k + j) * 2 * length_z, 2 * length_z), :] = out[:, j * lanes : (j + 1) * lanes]
        return carry

    lax.fori_loop(0, length_x // 2, step, 0, unroll=4)


def conv_body(
    left, mid, right, own, spec, ty_h, ty_l, fx_h, fx_l, fz_h, fz_l, gz_h, gz_l, gx_h, gx_l, iy_h, iy_l,
    *rest, brick, dims, lanes, groups, conj,
):
    outs, (s1, s2, s3, s4) = rest[:-4], rest[-4:]
    brick_z, brick_x, brick_y = brick
    length_z, length_x, length_y = dims
    rows = brick_z * brick_x
    chunk = rows // groups
    block = rows + chunk
    for g in range(groups):
        table = (ty_h[g], ty_l[g])
        for bx, ref in enumerate((left, mid, right)):
            data = jnp.concatenate(
                [
                    jnp.concatenate(
                        [ref[pl.ds(b * block + g * chunk, chunk), :], ref[pl.ds(b * block + rows, chunk), :]],
                        axis=1,
                    )
                    for b in range(3)
                ],
                axis=0,
            )
            out = dot3(split(data), table)
            per = chunk // brick_x
            for b in range(3):
                for zi in range(per):
                    z = b * brick_z + g * per + zi
                    src = b * chunk + zi * brick_x
                    s1[pl.ds(z * length_x + bx * brick_x, brick_x), :] = out[src : src + brick_x]
    transform_x(s1, s2, (fx_h[...], fx_l[...]), length_z, length_x, length_x, lanes)
    fz = (fz_h[...], fz_l[...])
    gz = (gz_h[...], gz_l[...])

    def middle(i, carry):
        k = i * 2
        data = jnp.concatenate(
            [pair_strided(s2, k + j, length_x, length_z, 2 * length_x) for j in range(2)], axis=1
        )
        out = dot3(fz, split(data))
        kern = jnp.concatenate(
            [spec[pl.ds((k + j) * 2 * length_z, 2 * length_z), :] for j in range(2)], axis=1
        )
        re, im = out[:length_z], out[length_z:]
        kr, ki = kern[:length_z], kern[length_z:]
        if conj:
            prod = jnp.concatenate([re * kr + im * ki, im * kr - re * ki], axis=0)
        else:
            prod = jnp.concatenate([re * kr - im * ki, re * ki + im * kr], axis=0)
        back = dot3(gz, split(prod))
        for j in range(2):
            s3[pl.ds((k + j) * 2 * brick_z, 2 * brick_z), :] = back[:, j * lanes : (j + 1) * lanes]
        return carry

    lax.fori_loop(0, length_x // 2, middle, 0, unroll=4)
    gx = (gx_h[...], gx_l[...])
    for z in range(0, brick_z, 2):
        data = jnp.concatenate(
            [pair_strided(s3, z + j, brick_z, length_x, 2 * brick_z) for j in range(2)], axis=1
        )
        out = dot3(gx, split(data))
        for j in range(2):
            part = out[:, j * lanes : (j + 1) * lanes]
            s4[pl.ds((z + j) * brick_x, brick_x), :lanes] = part[:brick_x]
            s4[pl.ds((z + j) * brick_x, brick_x), lanes:] = part[brick_x:]
    value = dot3(split(s4[...]), (iy_h[...], iy_l[...]))
    if conj:
        updated = own[...] * value
        cube = updated.reshape(brick_z, brick_x, brick_y)
        outs[0][...] = updated
        outs[1][...] = jnp.max(cube, axis=1)
        outs[2][...] = jnp.max(cube, axis=0)
        outs[3][...] = jnp.max(cube, axis=2)
    else:
        ratio = own[...] / value
        outs[0][...] = ratio
        outs[1][...] = packed_edges(ratio, groups)


def packed_edges(value, groups):
    rows, lanes = value.shape
    chunk = rows // groups
    width = lanes // groups
    lane = lax.broadcasted_iota(jnp.int32, (chunk, lanes), 1)
    out = pltpu.roll(value[:chunk], width // 2, 1)
    for g in range(1, groups):
        moved = pltpu.roll(value[g * chunk : (g + 1) * chunk], (width // 2 + g * width) % lanes, 1)
        out = jnp.where(lane >= g * width, moved, out)
    return out


def pack_body(value, out, *, groups):
    out[...] = packed_edges(value[...], groups)


def both_ways(value, axis):
    ends = lax.axis_size(axis) - 1
    ahead = lax.ppermute(value, axis, [(i, i + 1) for i in range(ends)])
    behind = lax.ppermute(value, axis, [(i + 1, i) for i in range(ends)])
    return ahead, behind


def surround(value, edges, margin):
    before, after = both_ways(edges, "gy")
    lane = lax.broadcasted_iota(jnp.int32, edges.shape, 1)
    halo = jnp.where(lane % (2 * margin) < margin, before, after)
    block = jnp.concatenate([value, halo], axis=0)
    low, high = both_ways(block, "gz")
    mid = jnp.concatenate([low, block, high], axis=0)
    left, right = both_ways(mid, "gx")
    return left, mid, right


def ring_max(value, axis):
    count = lax.axis_size(axis)
    if count <= 4:
        others = [
            lax.ppermute(value, axis, [(i, (i + s) % count) for i in range(count)]) for s in range(1, count)
        ]
        return functools.reduce(jnp.maximum, others, value)
    shift = 1
    while shift < count:
        moved = lax.ppermute(value, axis, [(i, (i + shift) % count) for i in range(count)])
        value = jnp.maximum(value, moved)
        shift *= 2
    return value


def shards(estimate, measured, point_spread):
    extent = point_spread.shape[0]
    margin = extent // 2
    brick = brick_z, brick_x, brick_y = estimate.shape
    assert brick_z == margin and brick_x == margin
    dims = length_z, length_x, length_y = tuple(n + extent for n in brick)
    lanes = -(-(length_y // 2 + 1) // 128) * 128
    groups = brick_y // extent
    rows = brick_z * brick_x
    chunk = rows // groups
    around_y = forward_right(length_y, np.arange(length_y), lanes)
    tables = np.zeros((groups, 2 * brick_y, 2 * lanes))
    for g in range(groups):
        tables[g, :brick_y] = around_y[margin : margin + brick_y]
        base = brick_y + g * extent
        tables[g, base : base + margin] = around_y[:margin]
        tables[g, base + margin : base + extent] = around_y[margin + brick_y :]
    inner = lambda n: np.arange(n) + margin
    conv_tables = (
        *constant(tables),
        *constant(forward_left(length_x, np.arange(length_x))),
        *constant(forward_left(length_z, np.arange(length_z))),
        *constant(inverse_left(length_z, inner(brick_z))),
        *constant(inverse_left(length_x, inner(brick_x))),
        *constant(inverse_right(length_y, inner(brick_y), lanes)),
    )
    offsets = np.arange(extent) - margin
    psf_tables = (
        *constant(forward_right(length_y, offsets, lanes)),
        *constant(forward_left(length_x, offsets)),
        *constant(forward_left(length_z, offsets)),
    )
    shape = jax.ShapeDtypeStruct
    scratch = lambda *s: pltpu.VMEM(s, F32)

    own = estimate.reshape(rows, brick_y)
    edges = pl.pallas_call(
        functools.partial(pack_body, groups=groups), out_shape=shape((chunk, brick_y), F32)
    )(own)
    spec = pl.pallas_call(
        functools.partial(spectrum_body, extent=extent, dims=dims, lanes=lanes),
        out_shape=shape((length_x * 2 * length_z, lanes), F32),
        scratch_shapes=[scratch(extent * extent, 2 * lanes), scratch(extent * 2 * length_x, lanes)],
    )(point_spread.reshape(extent * extent, extent), *psf_tables)

    def convolve(region, mate, conj, out_shape):
        return pl.pallas_call(
            functools.partial(conv_body, brick=brick, dims=dims, lanes=lanes, groups=groups, conj=conj),
            out_shape=out_shape,
            scratch_shapes=[
                scratch(length_z * length_x, 2 * lanes),
                scratch(length_z * 2 * length_x, lanes),
                scratch(length_x * 2 * brick_z, lanes),
                scratch(rows, 2 * lanes),
            ],
        )(*region, mate, spec, *conv_tables)

    ratio, ratio_edges = convolve(
        surround(own, edges, margin),
        measured.reshape(rows, brick_y),
        False,
        (shape((rows, brick_y), F32), shape((chunk, brick_y), F32)),
    )
    updated, across, top, along = convolve(
        surround(ratio, ratio_edges, margin),
        own,
        True,
        (
            shape((rows, brick_y), F32),
            shape((brick_z, brick_y), F32),
            shape((brick_x, brick_y), F32),
            shape((brick_z, brick_x), F32),
        ),
    )
    across = ring_max(across, "gx")
    along = ring_max(along, "gy")
    merged = ring_max(top, "gz")
    piece = brick_y // lax.axis_size("gz")
    top_view = lax.dynamic_slice_in_dim(merged, lax.axis_index("gz") * piece, piece, 1)
    return (updated.reshape(brick), across, along, top_view)


def solution(mesh):
    in_specs = (P("gz", "gx", "gy"), P("gz", "gx", "gy"), P())
    out_specs = (P("gz", "gx", "gy"), P("gz", "gy"), P("gz", "gx"), P("gx", ("gy", "gz")))
    return jax.shard_map(shards, mesh=mesh, in_specs=in_specs, out_specs=out_specs, check_vma=False)
```

```python
import functools

import jax
import jax.numpy as jnp
import numpy as np
from jax import lax
from jax.experimental import pallas as pl
from jax.experimental.pallas import tpu as pltpu
from jax.sharding import PartitionSpec as P

F32 = jnp.float32
BF16 = jnp.bfloat16


def split(value):
    high = value.astype(BF16)
    return high, (value - high.astype(F32)).astype(BF16)


def constant(table):
    table = np.asarray(table, np.float32)
    high = table.astype(BF16)
    low = (table - high.astype(np.float32)).astype(BF16)
    return high, low


def stacked(table):
    return jnp.asarray(np.concatenate(constant(table), axis=-2))


def mul(left, right):
    return jnp.dot(left, right, preferred_element_type=F32)


def table_dot(table, data):
    high, low = split(data)
    half = table.shape[0] // 2
    out = mul(table, high)
    return out[:half] + (out[half:] + mul(table[:half], low))


def dot_table(data, table_high, table_low):
    both = jnp.concatenate(split(data), axis=0)
    half = data.shape[0]
    out = mul(both, table_high)
    return out[:half] + (out[half:] + mul(both[:half], table_low))


def angles(rows, cols, length):
    return np.mod(np.outer(rows, cols), length) * (2.0 * np.pi / length)


def forward_left(length, positions):
    theta = angles(np.arange(length), positions, length)
    c, s = np.cos(theta), np.sin(theta)
    return np.block([[c, s], [-s, c]])


def inverse_left(length, positions):
    theta = angles(positions, np.arange(length), length)
    c, s = np.cos(theta), np.sin(theta)
    return np.block([[c, -s], [s, c]])


def forward_right(length, positions, lanes):
    count = length // 2 + 1
    theta = angles(positions, np.arange(count), length)
    out = np.zeros((len(positions), 2 * lanes))
    out[:, :count] = np.cos(theta)
    out[:, lanes : lanes + count] = -np.sin(theta)
    return out


def inverse_right(length, positions, lanes):
    count = length // 2 + 1
    freq = np.arange(count)
    weight = np.where((freq == 0) | (2 * freq == length), 1.0, 2.0)[:, None]
    theta = angles(freq, positions, length)
    out = np.zeros((2 * lanes, len(positions)))
    out[:count] = weight * np.cos(theta)
    out[lanes : lanes + count] = -weight * np.sin(theta)
    return out


def pair_x(s1, row, rows, lanes):
    block = s1[pl.ds(row, rows), :]
    return jnp.concatenate([block[:, :lanes], block[:, lanes:]], axis=0)


def pair_strided(ref, start, gap, rows, stride):
    return jnp.concatenate(
        [ref[pl.ds(start, rows, stride=stride), :], ref[pl.ds(start + gap, rows, stride=stride), :]], axis=0
    )


def transform_x(s1, s2, table, count_z, count_x, length_x, lanes):
    def step(i, carry):
        z = i * 2
        data = jnp.concatenate(
            [pair_x(s1, (z + j) * count_x, count_x, lanes) for j in range(2)], axis=1
        )
        out = table_dot(table, data)
        for j in range(2):
            s2[pl.ds((z + j) * 2 * length_x, 2 * length_x), :] = out[:, j * lanes : (j + 1) * lanes]
        return carry

    lax.fori_loop(0, count_z // 2, step, 0, unroll=4)


def spectrum_body(psf, ty_h, ty_l, fx, fz, spec, s1, s2, *, extent, dims, lanes):
    length_z, length_x, length_y = dims
    values = psf[...]
    scale = 1.0 / (jnp.sum(values) * float(length_z * length_x * length_y))
    s1[...] = dot_table(values, ty_h[...], ty_l[...]) * scale
    transform_x(s1, s2, fx[...], extent, extent, length_x, lanes)
    table = fz[...]

    def step(i, carry):
        k = i * 2
        data = jnp.concatenate(
            [pair_strided(s2, k + j, length_x, extent, 2 * length_x) for j in range(2)], axis=1
        )
        out = table_dot(table, data)
        for j in range(2):
            spec[pl.ds((k + j) * 2 * length_z, 2 * length_z), :] = out[:, j * lanes : (j + 1) * lanes]
        return carry

    lax.fori_loop(0, length_x // 2, step, 0, unroll=4)


def conv_body(place, *refs, brick, dims, lanes, groups, parts, conj):
    parts_z, parts_x = parts
    count = parts_z * parts_x
    region, refs = refs[:count], refs[count:]
    own, spec, ty_h, ty_l, fx, fz, gz, gx, iy_h, iy_l = refs[:10]
    outs, (s1, s2, s3, s4) = refs[10:-4], refs[-4:]
    brick_z, brick_x, brick_y = brick
    length_z, length_x, length_y = dims
    rows = brick_z * brick_x
    chunk = rows // groups
    per = chunk // brick_x
    wide_z, wide_x = parts_z * brick_z, parts_x * brick_x
    for g in range(groups):
        data = jnp.concatenate(
            [
                jnp.concatenate([ref[pl.ds(g * chunk, chunk), :], ref[pl.ds(rows, chunk), :]], axis=1)
                for ref in region
            ],
            axis=0,
        )
        out = dot_table(data, ty_h[g], ty_l[g])
        for n in range(count):
            bz, bx = n // parts_x, n % parts_x
            for zi in range(per):
                z = bz * brick_z + g * per + zi
                src = n * chunk + zi * brick_x
                s1[pl.ds(z * wide_x + bx * brick_x, brick_x), :] = out[src : src + brick_x]
    transform_x(s1, s2, fx[place[0]], wide_z, wide_x, length_x, lanes)
    forward_z = fz[place[1]]
    back_z = gz[...]

    def middle(i, carry):
        k = i * 2
        data = jnp.concatenate(
            [pair_strided(s2, k + j, length_x, wide_z, 2 * length_x) for j in range(2)], axis=1
        )
        out = table_dot(forward_z, data)
        kern = jnp.concatenate(
            [spec[pl.ds((k + j) * 2 * length_z, 2 * length_z), :] for j in range(2)], axis=1
        )
        re, im = out[:length_z], out[length_z:]
        kr, ki = kern[:length_z], kern[length_z:]
        if conj:
            prod = jnp.concatenate([re * kr + im * ki, im * kr - re * ki], axis=0)
        else:
            prod = jnp.concatenate([re * kr - im * ki, re * ki + im * kr], axis=0)
        back = table_dot(back_z, prod)
        for j in range(2):
            s3[pl.ds((k + j) * 2 * brick_z, 2 * brick_z), :] = back[:, j * lanes : (j + 1) * lanes]
        return carry

    lax.fori_loop(0, length_x // 2, middle, 0, unroll=4)
    back_x = gx[...]
    for z in range(0, brick_z, 2):
        data = jnp.concatenate(
            [pair_strided(s3, z + j, brick_z, length_x, 2 * brick_z) for j in range(2)], axis=1
        )
        out = table_dot(back_x, data)
        for j in range(2):
            part = out[:, j * lanes : (j + 1) * lanes]
            s4[pl.ds((z + j) * brick_x, brick_x), :lanes] = part[:brick_x]
            s4[pl.ds((z + j) * brick_x, brick_x), lanes:] = part[brick_x:]
    value = dot_table(s4[...], iy_h[...], iy_l[...])
    if conj:
        updated = own[...] * value
        cube = updated.reshape(brick_z, brick_x, brick_y)
        outs[0][...] = updated
        outs[1][...] = jnp.max(cube, axis=1)
        outs[2][...] = jnp.max(cube, axis=0)
        outs[3][...] = jnp.max(cube, axis=2)
    else:
        ratio = own[...] / value
        outs[0][...] = ratio
        outs[1][...] = packed_edges(ratio, groups)


def packed_edges(value, groups):
    rows, lanes = value.shape
    chunk = rows // groups
    width = lanes // groups
    lane = lax.broadcasted_iota(jnp.int32, (chunk, lanes), 1)
    out = pltpu.roll(value[:chunk], width // 2, 1)
    for g in range(1, groups):
        moved = pltpu.roll(value[g * chunk : (g + 1) * chunk], (width // 2 + g * width) % lanes, 1)
        out = jnp.where(lane >= g * width, moved, out)
    return out


def pack_body(value, out, *, groups):
    out[...] = packed_edges(value[...], groups)


def swaps(value, axis):
    count = lax.axis_size(axis)
    found = []
    for first in range(min(2, count - 1)):
        pairs = [(i, i + 1) for i in range(first, count - 1, 2)]
        found.append(lax.ppermute(value, axis, pairs + [(j, i) for i, j in pairs]))
    return found


def surround(value, edges, margin):
    sides = swaps(edges, "gy") + [jnp.zeros_like(edges)] * 2
    lane = lax.broadcasted_iota(jnp.int32, edges.shape, 1)
    odd = lax.axis_index("gy") % 2 == 1
    halo = jnp.where((lane % (2 * margin) < margin) == odd, sides[0], sides[1])
    block = jnp.concatenate([value, halo], axis=0)
    above = swaps(block, "gz")
    around = swaps(block, "gx")
    region = [block, *around]
    for part in above:
        region += [part, *swaps(part, "gx")]
    return region


def spots(count, brick, margin):
    own, low, high = np.arange(brick) + margin, np.arange(margin), np.arange(margin) + margin + brick
    kept = min(3, count)
    return [np.concatenate([own, high, low][:kept]), np.concatenate([own, low, high][:kept])]


def all_max(items):
    items = list(items)
    shift = 1
    while any(shift < lax.axis_size(axis) for _, axis in items):
        moved = []
        for value, axis in items:
            count = lax.axis_size(axis)
            if shift < count:
                pairs = [(i, (i + shift) % count) for i in range(count)]
                if count & (count - 1) == 0:
                    pairs = [(i, i ^ shift) for i in range(count)]
                moved.append(lax.ppermute(value, axis, pairs))
            else:
                moved.append(value)
        items = [(jnp.maximum(value, new), axis) for (value, axis), new in zip(items, moved)]
        shift *= 2
    return [value for value, _ in items]


def shards(estimate, measured, point_spread):
    extent = point_spread.shape[0]
    margin = extent // 2
    brick = brick_z, brick_x, brick_y = estimate.shape
    assert brick_z == margin and brick_x == margin
    dims = length_z, length_x, length_y = tuple(n + extent for n in brick)
    lanes = -(-(length_y // 2 + 1) // 128) * 128
    groups = brick_y // extent
    rows = brick_z * brick_x
    chunk = rows // groups
    around_y = forward_right(length_y, np.arange(length_y), lanes)
    tables = np.zeros((groups, 2 * brick_y, 2 * lanes))
    for g in range(groups):
        tables[g, :brick_y] = around_y[margin : margin + brick_y]
        base = brick_y + g * extent
        tables[g, base : base + margin] = around_y[:margin]
        tables[g, base + margin : base + extent] = around_y[margin + brick_y :]
    inner = lambda n: np.arange(n) + margin
    parts = parts_z, parts_x = tuple(min(3, lax.axis_size(axis)) for axis in ("gz", "gx"))
    spots_x = spots(lax.axis_size("gx"), brick_x, margin)
    spots_z = spots(lax.axis_size("gz"), brick_z, margin)
    conv_tables = (
        *map(jnp.asarray, constant(tables)),
        stacked(np.stack([forward_left(length_x, spot) for spot in spots_x])),
        stacked(np.stack([forward_left(length_z, spot) for spot in spots_z])),
        stacked(inverse_left(length_z, inner(brick_z))),
        stacked(inverse_left(length_x, inner(brick_x))),
        *map(jnp.asarray, constant(inverse_right(length_y, inner(brick_y), lanes))),
    )
    offsets = np.arange(extent) - margin
    psf_tables = (
        *map(jnp.asarray, constant(forward_right(length_y, offsets, lanes))),
        stacked(forward_left(length_x, offsets)),
        stacked(forward_left(length_z, offsets)),
    )
    place = jnp.stack([lax.axis_index("gx") % 2, lax.axis_index("gz") % 2]).astype(jnp.int32)
    shape = jax.ShapeDtypeStruct
    scratch = lambda *s: pltpu.VMEM(s, F32)

    own = estimate.reshape(rows, brick_y)
    edges = pl.pallas_call(
        functools.partial(pack_body, groups=groups), out_shape=shape((chunk, brick_y), F32)
    )(own)
    spec = pl.pallas_call(
        functools.partial(spectrum_body, extent=extent, dims=dims, lanes=lanes),
        out_shape=shape((length_x * 2 * length_z, lanes), F32),
        scratch_shapes=[scratch(extent * extent, 2 * lanes), scratch(extent * 2 * length_x, lanes)],
    )(point_spread.reshape(extent * extent, extent), *psf_tables)

    def convolve(region, mate, conj, out_shape):
        return pl.pallas_call(
            functools.partial(conv_body, brick=brick, dims=dims, lanes=lanes, groups=groups, parts=parts, conj=conj),
            out_shape=out_shape,
            in_specs=[pl.BlockSpec(memory_space=pltpu.SMEM)]
            + [pl.BlockSpec(memory_space=pltpu.VMEM)] * (len(region) + 2 + len(conv_tables)),
            scratch_shapes=[
                scratch(parts_z * brick_z * parts_x * brick_x, 2 * lanes),
                scratch(parts_z * brick_z * 2 * length_x, lanes),
                scratch(length_x * 2 * brick_z, lanes),
                scratch(rows, 2 * lanes),
            ],
        )(place, *region, mate, spec, *conv_tables)

    ratio, ratio_edges = convolve(
        surround(own, edges, margin),
        measured.reshape(rows, brick_y),
        False,
        (shape((rows, brick_y), F32), shape((chunk, brick_y), F32)),
    )
    updated, across, top, along = convolve(
        surround(ratio, ratio_edges, margin),
        own,
        True,
        (
            shape((rows, brick_y), F32),
            shape((brick_z, brick_y), F32),
            shape((brick_x, brick_y), F32),
            shape((brick_z, brick_x), F32),
        ),
    )
    merged, across, along = all_max([(top, "gz"), (across, "gx"), (along, "gy")])
    piece = brick_y // lax.axis_size("gz")
    top_view = lax.dynamic_slice_in_dim(merged, lax.axis_index("gz") * piece, piece, 1)
    return (updated.reshape(brick), across, along, top_view)


def solution(mesh):
    in_specs = (P("gz", "gx", "gy"), P("gz", "gx", "gy"), P())
    out_specs = (P("gz", "gx", "gy"), P("gz", "gy"), P("gz", "gx"), P("gx", ("gy", "gz")))
    return jax.shard_map(shards, mesh=mesh, in_specs=in_specs, out_specs=out_specs, check_vma=False)
```

```python
import functools

import jax
import jax.numpy as jnp
import numpy as np
from jax import lax
from jax.experimental import pallas as pl
from jax.experimental.pallas import tpu as pltpu
from jax.sharding import PartitionSpec as P

F32 = jnp.float32
BF16 = jnp.bfloat16
UNROLL = 8


def split(value):
    high = value.astype(BF16)
    return high, (value - high.astype(F32)).astype(BF16)


def constant(table):
    table = np.asarray(table, np.float32)
    high = table.astype(BF16)
    low = (table - high.astype(np.float32)).astype(BF16)
    return high, low


def stacked(table):
    return jnp.asarray(np.concatenate(constant(table), axis=-2))


def mul(left, right):
    return jnp.dot(left, right, preferred_element_type=F32)


def table_dot(table, data):
    high, low = split(data)
    half = table.shape[0] // 2
    out = mul(table, high)
    return out[:half] + (out[half:] + mul(table[:half], low))


def dot_table(data, table_high, table_low):
    both = jnp.concatenate(split(data), axis=0)
    half = data.shape[0]
    out = mul(both, table_high)
    return out[:half] + (out[half:] + mul(both[:half], table_low))


def angles(rows, cols, length):
    return np.mod(np.outer(rows, cols), length) * (2.0 * np.pi / length)


def forward_left(length, positions):
    theta = angles(np.arange(length), positions, length)
    c, s = np.cos(theta), np.sin(theta)
    return np.block([[c, s], [-s, c]])


def inverse_left(length, positions):
    theta = angles(positions, np.arange(length), length)
    c, s = np.cos(theta), np.sin(theta)
    return np.block([[c, -s], [s, c]])


def forward_right(length, positions, lanes):
    count = length // 2 + 1
    theta = angles(positions, np.arange(count), length)
    out = np.zeros((len(positions), 2 * lanes))
    out[:, :count] = np.cos(theta)
    out[:, lanes : lanes + count] = -np.sin(theta)
    return out


def inverse_right(length, positions, lanes):
    count = length // 2 + 1
    freq = np.arange(count)
    weight = np.where((freq == 0) | (2 * freq == length), 1.0, 2.0)[:, None]
    theta = angles(freq, positions, length)
    out = np.zeros((2 * lanes, len(positions)))
    out[:count] = weight * np.cos(theta)
    out[lanes : lanes + count] = -weight * np.sin(theta)
    return out


def pair_x(s1, row, rows, lanes):
    block = s1[pl.ds(row, rows), :]
    return jnp.concatenate([block[:, :lanes], block[:, lanes:]], axis=0)


def pair_strided(ref, start, gap, rows, stride):
    return jnp.concatenate(
        [ref[pl.ds(start, rows, stride=stride), :], ref[pl.ds(start + gap, rows, stride=stride), :]], axis=0
    )


def transform_x(s1, s2, table, count_z, count_x, length_x, lanes):
    def step(i, carry):
        z = i * 2
        data = jnp.concatenate(
            [pair_x(s1, (z + j) * count_x, count_x, lanes) for j in range(2)], axis=1
        )
        out = table_dot(table, data)
        for j in range(2):
            s2[pl.ds((z + j) * 2 * length_x, 2 * length_x), :] = out[:, j * lanes : (j + 1) * lanes]
        return carry

    lax.fori_loop(0, count_z // 2, step, 0, unroll=UNROLL)


def spectrum_body(psf, ty_h, ty_l, fx, fz, spec, s1, s2, *, extent, dims, lanes):
    length_z, length_x, length_y = dims
    width = ty_h.shape[1]
    per = width // extent
    tiles = extent // per
    values = psf[...]
    scale = 1.0 / (jnp.sum(values) * float(length_z * length_x * length_y))
    data = jnp.concatenate([values[:, t * width : (t + 1) * width] for t in range(tiles)], axis=0)
    for g in range(per):
        out = dot_table(data, ty_h[g], ty_l[g]) * scale
        for t in range(tiles):
            s1[pl.ds((t * per + g) * extent, extent), :] = out[t * extent : (t + 1) * extent]
    transform_x(s1, s2, fz[...], extent, extent, length_z, lanes)
    table = fx[...]

    def step(i, carry):
        q = i * 2
        data = jnp.concatenate(
            [pair_strided(s2, q + j, length_z, extent, 2 * length_z) for j in range(2)], axis=1
        )
        out = table_dot(table, data)
        for j in range(2):
            part = out[:, j * lanes : (j + 1) * lanes]
            spec[pl.ds(q + j, length_x, stride=2 * length_z), :] = part[:length_x]
            spec[pl.ds(length_z + q + j, length_x, stride=2 * length_z), :] = part[length_x:]
        return carry

    lax.fori_loop(0, length_z // 2, step, 0, unroll=UNROLL)


def conv_body(*refs, brick, dims, lanes, groups, parts, conj):
    parts_z, parts_x = parts
    count = parts_z * parts_x
    region, refs = refs[:count], refs[count:]
    own, spec, ty_h, ty_l, fx, fz, gz, gx, iy_h, iy_l = refs[:10]
    outs, (s1, s2, s3, s4) = refs[10:-4], refs[-4:]
    brick_z, brick_x, brick_y = brick
    length_z, length_x, length_y = dims
    rows = brick_z * brick_x
    chunk = rows // groups
    per = chunk // brick_x
    wide_z, wide_x = parts_z * brick_z, parts_x * brick_x
    for g in range(groups):
        data = jnp.concatenate(
            [
                jnp.concatenate([ref[pl.ds(g * chunk, chunk), :], ref[pl.ds(rows, chunk), :]], axis=1)
                for ref in region
            ],
            axis=0,
        )
        out = dot_table(data, ty_h[g], ty_l[g])
        for n in range(count):
            bz, bx = n // parts_x, n % parts_x
            for zi in range(per):
                z = bz * brick_z + g * per + zi
                src = n * chunk + zi * brick_x
                s1[pl.ds(z * wide_x + bx * brick_x, brick_x), :] = out[src : src + brick_x]
    transform_x(s1, s2, fx[lax.axis_index("gx") % 2], wide_z, wide_x, length_x, lanes)
    forward_z = fz[lax.axis_index("gz") % 2]
    back_z = gz[...]

    def middle(i, carry):
        k = i * 2
        data = jnp.concatenate(
            [pair_strided(s2, k + j, length_x, wide_z, 2 * length_x) for j in range(2)], axis=1
        )
        out = table_dot(forward_z, data)
        kern = jnp.concatenate(
            [spec[pl.ds((k + j) * 2 * length_z, 2 * length_z), :] for j in range(2)], axis=1
        )
        re, im = out[:length_z], out[length_z:]
        kr, ki = kern[:length_z], kern[length_z:]
        if conj:
            prod = jnp.concatenate([re * kr + im * ki, im * kr - re * ki], axis=0)
        else:
            prod = jnp.concatenate([re * kr - im * ki, re * ki + im * kr], axis=0)
        back = table_dot(back_z, prod)
        for j in range(2):
            s3[pl.ds((k + j) * 2 * brick_z, 2 * brick_z), :] = back[:, j * lanes : (j + 1) * lanes]
        return carry

    lax.fori_loop(0, length_x // 2, middle, 0, unroll=UNROLL)
    back_x = gx[...]
    for z in range(0, brick_z, 2):
        data = jnp.concatenate(
            [pair_strided(s3, z + j, brick_z, length_x, 2 * brick_z) for j in range(2)], axis=1
        )
        out = table_dot(back_x, data)
        for j in range(2):
            part = out[:, j * lanes : (j + 1) * lanes]
            s4[pl.ds((z + j) * brick_x, brick_x), :lanes] = part[:brick_x]
            s4[pl.ds((z + j) * brick_x, brick_x), lanes:] = part[brick_x:]
    value = dot_table(s4[...], iy_h[...], iy_l[...])
    if conj:
        updated = own[...] * value
        cube = updated.reshape(brick_z, brick_x, brick_y)
        outs[0][...] = updated
        outs[1][...] = jnp.max(cube, axis=1)
        outs[2][...] = jnp.max(cube, axis=0)
        outs[3][...] = jnp.max(cube, axis=2)
    else:
        ratio = own[...] / value
        outs[0][...] = ratio
        outs[1][...] = packed_edges(ratio, groups)


def packed_edges(value, groups):
    rows, lanes = value.shape
    chunk = rows // groups
    width = lanes // groups
    lane = lax.broadcasted_iota(jnp.int32, (chunk, lanes), 1)
    out = pltpu.roll(value[:chunk], width // 2, 1)
    for g in range(1, groups):
        moved = pltpu.roll(value[g * chunk : (g + 1) * chunk], (width // 2 + g * width) % lanes, 1)
        out = jnp.where(lane >= g * width, moved, out)
    return out


def pack_body(value, out, *, groups):
    out[...] = packed_edges(value[...], groups)


def swaps(value, axis):
    count = lax.axis_size(axis)
    found = []
    for first in range(min(2, count - 1)):
        pairs = [(i, i + 1) for i in range(first, count - 1, 2)]
        found.append(lax.ppermute(value, axis, pairs + [(j, i) for i, j in pairs]))
    return found


def surround(value, edges, margin):
    sides = swaps(edges, "gy") + [jnp.zeros_like(edges)] * 2
    lane = lax.broadcasted_iota(jnp.int32, edges.shape, 1)
    odd = lax.axis_index("gy") % 2 == 1
    halo = jnp.where((lane % (2 * margin) < margin) == odd, sides[0], sides[1])
    block = jnp.concatenate([value, halo], axis=0)
    above = swaps(block, "gz")
    around = swaps(block, "gx")
    region = [block, *around]
    for part in above:
        region += [part, *swaps(part, "gx")]
    return region


def spots(count, brick, margin):
    own, low, high = np.arange(brick) + margin, np.arange(margin), np.arange(margin) + margin + brick
    kept = min(3, count)
    return [np.concatenate([own, high, low][:kept]), np.concatenate([own, low, high][:kept])]


def all_max(items):
    items = list(items)
    shift = 1
    while any(shift < lax.axis_size(axis) for _, axis in items):
        moved = []
        for value, axis in items:
            count = lax.axis_size(axis)
            if shift < count:
                pairs = [(i, (i + shift) % count) for i in range(count)]
                if count & (count - 1) == 0:
                    pairs = [(i, i ^ shift) for i in range(count)]
                moved.append(lax.ppermute(value, axis, pairs))
            else:
                moved.append(value)
        items = [(jnp.maximum(value, new), axis) for (value, axis), new in zip(items, moved)]
        shift *= 2
    return [value for value, _ in items]


def shards(estimate, measured, point_spread):
    extent = point_spread.shape[0]
    margin = extent // 2
    brick = brick_z, brick_x, brick_y = estimate.shape
    assert brick_z == margin and brick_x == margin
    dims = length_z, length_x, length_y = tuple(n + extent for n in brick)
    lanes = -(-(length_y // 2 + 1) // 128) * 128
    groups = brick_y // extent
    rows = brick_z * brick_x
    chunk = rows // groups
    around_y = forward_right(length_y, np.arange(length_y), lanes)
    tables = np.zeros((groups, 2 * brick_y, 2 * lanes))
    for g in range(groups):
        tables[g, :brick_y] = around_y[margin : margin + brick_y]
        base = brick_y + g * extent
        tables[g, base : base + margin] = around_y[:margin]
        tables[g, base + margin : base + extent] = around_y[margin + brick_y :]
    inner = lambda n: np.arange(n) + margin
    parts = parts_z, parts_x = tuple(min(3, lax.axis_size(axis)) for axis in ("gz", "gx"))
    spots_x = spots(lax.axis_size("gx"), brick_x, margin)
    spots_z = spots(lax.axis_size("gz"), brick_z, margin)
    conv_tables = (
        *map(jnp.asarray, constant(tables)),
        stacked(np.stack([forward_left(length_x, spot) for spot in spots_x])),
        stacked(np.stack([forward_left(length_z, spot) for spot in spots_z])),
        stacked(inverse_left(length_z, inner(brick_z))),
        stacked(inverse_left(length_x, inner(brick_x))),
        *map(jnp.asarray, constant(inverse_right(length_y, inner(brick_y), lanes))),
    )
    offsets = np.arange(extent) - margin
    per = max(1, 128 // extent)
    psf_y = np.zeros((per, per * extent, 2 * lanes))
    for g in range(per):
        psf_y[g, g * extent : (g + 1) * extent] = forward_right(length_y, offsets, lanes)
    psf_tables = (
        *map(jnp.asarray, constant(psf_y)),
        stacked(forward_left(length_x, offsets)),
        stacked(forward_left(length_z, offsets)),
    )
    shape = jax.ShapeDtypeStruct
    scratch = lambda *s: pltpu.VMEM(s, F32)

    own = estimate.reshape(rows, brick_y)
    edges = pl.pallas_call(
        functools.partial(pack_body, groups=groups), out_shape=shape((chunk, brick_y), F32)
    )(own)
    spec = pl.pallas_call(
        functools.partial(spectrum_body, extent=extent, dims=dims, lanes=lanes),
        out_shape=shape((length_x * 2 * length_z, lanes), F32),
        scratch_shapes=[scratch(extent * extent, 2 * lanes), scratch(extent * 2 * length_x, lanes)],
    )(point_spread, *psf_tables)

    def convolve(region, mate, conj, out_shape):
        return pl.pallas_call(
            functools.partial(conv_body, brick=brick, dims=dims, lanes=lanes, groups=groups, parts=parts, conj=conj),
            out_shape=out_shape,
            scratch_shapes=[
                scratch(parts_z * brick_z * parts_x * brick_x, 2 * lanes),
                scratch(parts_z * brick_z * 2 * length_x, lanes),
                scratch(length_x * 2 * brick_z, lanes),
                scratch(rows, 2 * lanes),
            ],
        )(*region, mate, spec, *conv_tables)

    ratio, ratio_edges = convolve(
        surround(own, edges, margin),
        measured.reshape(rows, brick_y),
        False,
        (shape((rows, brick_y), F32), shape((chunk, brick_y), F32)),
    )
    updated, across, top, along = convolve(
        surround(ratio, ratio_edges, margin),
        own,
        True,
        (
            shape((rows, brick_y), F32),
            shape((brick_z, brick_y), F32),
            shape((brick_x, brick_y), F32),
            shape((brick_z, brick_x), F32),
        ),
    )
    merged, across, along = all_max([(top, "gz"), (across, "gx"), (along, "gy")])
    piece = brick_y // lax.axis_size("gz")
    top_view = lax.dynamic_slice_in_dim(merged, lax.axis_index("gz") * piece, piece, 1)
    return (updated.reshape(brick), across, along, top_view)


def solution(mesh):
    in_specs = (P("gz", "gx", "gy"), P("gz", "gx", "gy"), P())
    out_specs = (P("gz", "gx", "gy"), P("gz", "gy"), P("gz", "gx"), P("gx", ("gy", "gz")))
    return jax.shard_map(shards, mesh=mesh, in_specs=in_specs, out_specs=out_specs, check_vma=False)
```

```python
import functools

import jax
import jax.numpy as jnp
import numpy as np
from jax import lax
from jax.experimental import pallas as pl
from jax.experimental.pallas import tpu as pltpu
from jax.sharding import PartitionSpec as P

F32 = jnp.float32
BF16 = jnp.bfloat16
UNROLL = 4
WIDE = 4


def split(value):
    high = value.astype(BF16)
    return high, (value - high.astype(F32)).astype(BF16)


def constant(table):
    table = np.asarray(table, np.float32)
    high = table.astype(BF16)
    low = (table - high.astype(np.float32)).astype(BF16)
    return high, low


def stacked(table):
    return jnp.asarray(np.concatenate(constant(table), axis=-2))


def mul(left, right):
    return jnp.dot(left, right, preferred_element_type=F32)


def table_dot(table, data):
    high, low = split(data)
    half = table.shape[0] // 2
    out = mul(table, high)
    return out[:half] + (out[half:] + mul(table[:half], low))


def dot_table(data, table_high, table_low):
    both = jnp.concatenate(split(data), axis=0)
    half = data.shape[0]
    out = mul(both, table_high)
    return out[:half] + (out[half:] + mul(both[:half], table_low))


def angles(rows, cols, length):
    return np.mod(np.outer(rows, cols), length) * (2.0 * np.pi / length)


def forward_left(length, positions):
    theta = angles(np.arange(length), positions, length)
    c, s = np.cos(theta), np.sin(theta)
    return np.block([[c, s], [-s, c]])


def inverse_left(length, positions):
    theta = angles(positions, np.arange(length), length)
    c, s = np.cos(theta), np.sin(theta)
    return np.block([[c, -s], [s, c]])


def forward_right(length, positions, lanes):
    count = length // 2 + 1
    theta = angles(positions, np.arange(count), length)
    out = np.zeros((len(positions), 2 * lanes))
    out[:, :count] = np.cos(theta)
    out[:, lanes : lanes + count] = -np.sin(theta)
    return out


def inverse_right(length, positions, lanes):
    count = length // 2 + 1
    freq = np.arange(count)
    weight = np.where((freq == 0) | (2 * freq == length), 1.0, 2.0)[:, None]
    theta = angles(freq, positions, length)
    out = np.zeros((2 * lanes, len(positions)))
    out[:count] = weight * np.cos(theta)
    out[lanes : lanes + count] = -weight * np.sin(theta)
    return out


def pair_x(s1, row, rows, lanes):
    block = s1[pl.ds(row, rows), :]
    return jnp.concatenate([block[:, :lanes], block[:, lanes:]], axis=0)


def pair_strided(ref, start, gap, rows, stride):
    return jnp.concatenate(
        [ref[pl.ds(start, rows, stride=stride), :], ref[pl.ds(start + gap, rows, stride=stride), :]], axis=0
    )


def transform_x(s1, s2, table, count_z, count_x, length_x, lanes):
    def step(i, carry):
        z = i * WIDE
        data = jnp.concatenate(
            [pair_x(s1, (z + j) * count_x, count_x, lanes) for j in range(WIDE)], axis=1
        )
        out = table_dot(table, data)
        for j in range(WIDE):
            s2[pl.ds((z + j) * 2 * length_x, 2 * length_x), :] = out[:, j * lanes : (j + 1) * lanes]
        return carry

    lax.fori_loop(0, count_z // WIDE, step, 0, unroll=UNROLL)


def spectrum_body(psf, ty_h, ty_l, fx, fz, spec, s1, s2, *, extent, dims, lanes):
    length_z, length_x, length_y = dims
    width = ty_h.shape[1]
    per = width // extent
    tiles = extent // per
    values = psf[...]
    scale = 1.0 / (jnp.sum(values) * float(length_z * length_x * length_y))
    data = jnp.concatenate([values[:, t * width : (t + 1) * width] for t in range(tiles)], axis=0)
    for g in range(per):
        out = dot_table(data, ty_h[g], ty_l[g]) * scale
        for t in range(tiles):
            s1[pl.ds((t * per + g) * extent, extent), :] = out[t * extent : (t + 1) * extent]
    transform_x(s1, s2, fz[...], extent, extent, length_z, lanes)
    table = fx[...]

    def step(i, carry):
        q = i * WIDE
        data = jnp.concatenate(
            [pair_strided(s2, q + j, length_z, extent, 2 * length_z) for j in range(WIDE)], axis=1
        )
        out = table_dot(table, data)
        for j in range(WIDE):
            part = out[:, j * lanes : (j + 1) * lanes]
            spec[pl.ds(q + j, length_x, stride=2 * length_z), :] = part[:length_x]
            spec[pl.ds(length_z + q + j, length_x, stride=2 * length_z), :] = part[length_x:]
        return carry

    lax.fori_loop(0, length_z // WIDE, step, 0, unroll=UNROLL)


def conv_body(*refs, brick, dims, lanes, groups, parts, conj):
    parts_z, parts_x = parts
    count = parts_z * parts_x
    region, refs = refs[:count], refs[count:]
    own, spec, ty_h, ty_l, fx, fz, gz, gx, iy_h, iy_l = refs[:10]
    outs, (s1, s2, s3, s4) = refs[10:-4], refs[-4:]
    brick_z, brick_x, brick_y = brick
    length_z, length_x, length_y = dims
    rows = brick_z * brick_x
    chunk = rows // groups
    per = chunk // brick_x
    wide_z, wide_x = parts_z * brick_z, parts_x * brick_x
    for g in range(groups):
        data = jnp.concatenate(
            [
                jnp.concatenate([ref[pl.ds(g * chunk, chunk), :], ref[pl.ds(rows, chunk), :]], axis=1)
                for ref in region
            ],
            axis=0,
        )
        out = dot_table(data, ty_h[g], ty_l[g])
        for n in range(count):
            bz, bx = n // parts_x, n % parts_x
            for zi in range(per):
                z = bz * brick_z + g * per + zi
                src = n * chunk + zi * brick_x
                s1[pl.ds(z * wide_x + bx * brick_x, brick_x), :] = out[src : src + brick_x]
    transform_x(s1, s2, fx[lax.axis_index("gx") % 2], wide_z, wide_x, length_x, lanes)
    forward_z = fz[lax.axis_index("gz") % 2]
    back_z = gz[...]

    def middle(i, carry):
        k = i * WIDE
        data = jnp.concatenate(
            [pair_strided(s2, k + j, length_x, wide_z, 2 * length_x) for j in range(WIDE)], axis=1
        )
        out = table_dot(forward_z, data)
        kern = jnp.concatenate(
            [spec[pl.ds((k + j) * 2 * length_z, 2 * length_z), :] for j in range(WIDE)], axis=1
        )
        re, im = out[:length_z], out[length_z:]
        kr, ki = kern[:length_z], kern[length_z:]
        if conj:
            prod = jnp.concatenate([re * kr + im * ki, im * kr - re * ki], axis=0)
        else:
            prod = jnp.concatenate([re * kr - im * ki, re * ki + im * kr], axis=0)
        back = table_dot(back_z, prod)
        for j in range(WIDE):
            s3[pl.ds((k + j) * 2 * brick_z, 2 * brick_z), :] = back[:, j * lanes : (j + 1) * lanes]
        return carry

    lax.fori_loop(0, length_x // WIDE, middle, 0, unroll=UNROLL)
    back_x = gx[...]
    for z in range(0, brick_z, WIDE):
        data = jnp.concatenate(
            [pair_strided(s3, z + j, brick_z, length_x, 2 * brick_z) for j in range(WIDE)], axis=1
        )
        out = table_dot(back_x, data)
        for j in range(WIDE):
            part = out[:, j * lanes : (j + 1) * lanes]
            s4[pl.ds((z + j) * brick_x, brick_x), :lanes] = part[:brick_x]
            s4[pl.ds((z + j) * brick_x, brick_x), lanes:] = part[brick_x:]
    value = dot_table(s4[...], iy_h[...], iy_l[...])
    if conj:
        updated = own[...] * value
        cube = updated.reshape(brick_z, brick_x, brick_y)
        outs[0][...] = updated
        outs[1][...] = jnp.max(cube, axis=1)
        outs[2][...] = jnp.max(cube, axis=0)
        outs[3][...] = jnp.max(cube, axis=2)
    else:
        ratio = own[...] / value
        outs[0][...] = ratio
        outs[1][...] = packed_edges(ratio, groups)


def packed_edges(value, groups):
    rows, lanes = value.shape
    chunk = rows // groups
    width = lanes // groups
    lane = lax.broadcasted_iota(jnp.int32, (chunk, lanes), 1)
    out = pltpu.roll(value[:chunk], width // 2, 1)
    for g in range(1, groups):
        moved = pltpu.roll(value[g * chunk : (g + 1) * chunk], (width // 2 + g * width) % lanes, 1)
        out = jnp.where(lane >= g * width, moved, out)
    return out


def pack_body(value, out, *, groups):
    out[...] = packed_edges(value[...], groups)


def swaps(value, axis):
    count = lax.axis_size(axis)
    found = []
    for first in range(min(2, count - 1)):
        pairs = [(i, i + 1) for i in range(first, count - 1, 2)]
        found.append(lax.ppermute(value, axis, pairs + [(j, i) for i, j in pairs]))
    return found


def surround(value, edges, margin):
    sides = swaps(edges, "gy") + [jnp.zeros_like(edges)] * 2
    lane = lax.broadcasted_iota(jnp.int32, edges.shape, 1)
    odd = lax.axis_index("gy") % 2 == 1
    halo = jnp.where((lane % (2 * margin) < margin) == odd, sides[0], sides[1])
    block = jnp.concatenate([value, halo], axis=0)
    above = swaps(block, "gz")
    around = swaps(block, "gx")
    region = [block, *around]
    for part in above:
        region += [part, *swaps(part, "gx")]
    return region


def spots(count, brick, margin):
    own, low, high = np.arange(brick) + margin, np.arange(margin), np.arange(margin) + margin + brick
    kept = min(3, count)
    return [np.concatenate([own, high, low][:kept]), np.concatenate([own, low, high][:kept])]


def all_max(items):
    items = list(items)
    shift = 1
    while any(shift < lax.axis_size(axis) for _, axis in items):
        moved = []
        for value, axis in items:
            count = lax.axis_size(axis)
            if shift < count:
                pairs = [(i, (i + shift) % count) for i in range(count)]
                if count & (count - 1) == 0:
                    pairs = [(i, i ^ shift) for i in range(count)]
                moved.append(lax.ppermute(value, axis, pairs))
            else:
                moved.append(value)
        items = [(jnp.maximum(value, new), axis) for (value, axis), new in zip(items, moved)]
        shift *= 2
    return [value for value, _ in items]


def shards(estimate, measured, point_spread):
    extent = point_spread.shape[0]
    margin = extent // 2
    brick = brick_z, brick_x, brick_y = estimate.shape
    assert brick_z == margin and brick_x == margin
    dims = length_z, length_x, length_y = tuple(n + extent for n in brick)
    lanes = -(-(length_y // 2 + 1) // 128) * 128
    groups = brick_y // extent
    rows = brick_z * brick_x
    chunk = rows // groups
    around_y = forward_right(length_y, np.arange(length_y), lanes)
    tables = np.zeros((groups, 2 * brick_y, 2 * lanes))
    for g in range(groups):
        tables[g, :brick_y] = around_y[margin : margin + brick_y]
        base = brick_y + g * extent
        tables[g, base : base + margin] = around_y[:margin]
        tables[g, base + margin : base + extent] = around_y[margin + brick_y :]
    inner = lambda n: np.arange(n) + margin
    parts = parts_z, parts_x = tuple(min(3, lax.axis_size(axis)) for axis in ("gz", "gx"))
    spots_x = spots(lax.axis_size("gx"), brick_x, margin)
    spots_z = spots(lax.axis_size("gz"), brick_z, margin)
    conv_tables = (
        *map(jnp.asarray, constant(tables)),
        stacked(np.stack([forward_left(length_x, spot) for spot in spots_x])),
        stacked(np.stack([forward_left(length_z, spot) for spot in spots_z])),
        stacked(inverse_left(length_z, inner(brick_z))),
        stacked(inverse_left(length_x, inner(brick_x))),
        *map(jnp.asarray, constant(inverse_right(length_y, inner(brick_y), lanes))),
    )
    offsets = np.arange(extent) - margin
    per = max(1, 128 // extent)
    psf_y = np.zeros((per, per * extent, 2 * lanes))
    for g in range(per):
        psf_y[g, g * extent : (g + 1) * extent] = forward_right(length_y, offsets, lanes)
    psf_tables = (
        *map(jnp.asarray, constant(psf_y)),
        stacked(forward_left(length_x, offsets)),
        stacked(forward_left(length_z, offsets)),
    )
    shape = jax.ShapeDtypeStruct
    scratch = lambda *s: pltpu.VMEM(s, F32)

    own = estimate.reshape(rows, brick_y)
    edges = pl.pallas_call(
        functools.partial(pack_body, groups=groups), out_shape=shape((chunk, brick_y), F32)
    )(own)
    spec = pl.pallas_call(
        functools.partial(spectrum_body, extent=extent, dims=dims, lanes=lanes),
        out_shape=shape((length_x * 2 * length_z, lanes), F32),
        scratch_shapes=[scratch(extent * extent, 2 * lanes), scratch(extent * 2 * length_x, lanes)],
    )(point_spread, *psf_tables)

    def convolve(region, mate, conj, out_shape):
        return pl.pallas_call(
            functools.partial(conv_body, brick=brick, dims=dims, lanes=lanes, groups=groups, parts=parts, conj=conj),
            out_shape=out_shape,
            scratch_shapes=[
                scratch(parts_z * brick_z * parts_x * brick_x, 2 * lanes),
                scratch(parts_z * brick_z * 2 * length_x, lanes),
                scratch(length_x * 2 * brick_z, lanes),
                scratch(rows, 2 * lanes),
            ],
        )(*region, mate, spec, *conv_tables)

    ratio, ratio_edges = convolve(
        surround(own, edges, margin),
        measured.reshape(rows, brick_y),
        False,
        (shape((rows, brick_y), F32), shape((chunk, brick_y), F32)),
    )
    updated, across, top, along = convolve(
        surround(ratio, ratio_edges, margin),
        own,
        True,
        (
            shape((rows, brick_y), F32),
            shape((brick_z, brick_y), F32),
            shape((brick_x, brick_y), F32),
            shape((brick_z, brick_x), F32),
        ),
    )
    merged, across, along = all_max([(top, "gz"), (across, "gx"), (along, "gy")])
    piece = brick_y // lax.axis_size("gz")
    top_view = lax.dynamic_slice_in_dim(merged, lax.axis_index("gz") * piece, piece, 1)
    return (updated.reshape(brick), across, along, top_view)


def solution(mesh):
    in_specs = (P("gz", "gx", "gy"), P("gz", "gx", "gy"), P())
    out_specs = (P("gz", "gx", "gy"), P("gz", "gy"), P("gz", "gx"), P("gx", ("gy", "gz")))
    return jax.shard_map(shards, mesh=mesh, in_specs=in_specs, out_specs=out_specs, check_vma=False)
```
